32 devices in a mesh: section: 2 (over x), row: 4 (over y, core), col: 4 (over z).
Axes of the slice: x: 2, y: 2, z: 4, core: 2. Of those that a mesh axis runs over, the one named last changes fastest.
Arguments:
- stash_inputs: bfloat16 [2, 4, 512, 12288], P('section', None, 'row', 'col'), may hold values from -16 to 16
- stash_hidden: bfloat16 [2, 4, 512, 24576], P('section', None, 'col', 'row'), may hold values from -6 to 6
- grad_in: bfloat16 [2, 512, 12288], P('section', 'row', 'col'), may hold values from -6 to 6
- w_in: bfloat16 [2, 12288, 24576], P('section', 'col', 'row'), may hold values from -0.0546875 to 0.0546875
- b_in: float32 [2, 24576], P('section', 'row'), may hold values from -3 to 3
- w_out: bfloat16 [2, 24576, 12288], P('section', 'row', 'col'), may hold values from -0.0390625 to 0.0390625
- b_out: float32 [2, 12288], P('section', 'col'), may hold values from -3 to 3
- ln_gain: float32 [2, 12288], P('section', 'col'), may hold values from 0.4 to 1.6
- plan: int32 [2, 2], P('section'), may hold values from 0 to 3, as said below
Outputs:
- act_recv: bfloat16 [2, 512, 12288], P('section', 'row', 'col')
- grad_recv: bfloat16 [2, 512, 12288], P('section', 'row', 'col')
- saved_hidden: bfloat16 [2, 512, 24576], P('section', 'col', 'row')
The draws below stay inside these ranges and needn't reach their ends.
Inputs may be any that keep to these rules, and one draw needn't show every extreme that they name: plan[s, 0] is the stash slot of the micro-batch that section s takes backward, plan[s, 1] that of the one it takes forward; the two differ.
All inputs are finite; a program needn't handle non-finite values.
Results may differ from the reference program's by a relative error of at most 0.015.
Values may be sent and summed in bfloat16 or wider, within the bound.
A program may use at most 192 MiB of HBM per device.

```python
import jax
import jax.numpy as jnp
from jax import lax

D = 12288
FF = 24576
TOK = 512
STASH = 4
N_SECTION = 2


def draw_stash_inputs(key, part):
    key_noise = jax.random.fold_in(key, 11)
    key_cols = jax.random.fold_in(key, 12)
    ramp = jnp.arange(D, dtype=jnp.float32) / D
    col_scale = jnp.exp(ramp * jnp.log(3.0) + jax.random.uniform(key_cols, (D,), jnp.float32, 0.0, jnp.log(4.0))) / 6.0
    noise = jnp.clip(jax.random.normal(key_noise, (N_SECTION, STASH, TOK, D), jnp.float32), -6.0, 6.0)
    values = noise * col_scale
    return values.astype(jnp.bfloat16)


def draw_plan(key, part):
    key_back = jax.random.fold_in(key, 21)
    key_step = jax.random.fold_in(key, 22)
    back_slot = jax.random.randint(key_back, (N_SECTION,), 0, STASH)
    step_size = jax.random.randint(key_step, (N_SECTION,), 1, STASH)
    fwd_slot = (back_slot + step_size) % STASH
    return jnp.stack([back_slot, fwd_slot], axis=1).astype(jnp.int32)


def levels(own_key, dims, pieces, smallest, largest):
    level = 1.0
    for dim, shards_of in pieces:
        steps = jax.random.uniform(jax.random.fold_in(jax.random.fold_in(own_key, 6), dim), (shards_of,), jnp.float32, smallest / len(pieces), largest / len(pieces))
        level = level * jnp.repeat(jnp.exp(steps), dims[dim] // shards_of).reshape((-1,) + (1,) * (len(dims) - 1 - dim))
    return level


def scatter_about(rng, shape, width, limit, pieces=(), held_as=jnp.bfloat16):
    drawn = jax.random.normal(rng, shape, jnp.float32) * width
    if len(pieces) > 0:
        drawn = levels(rng, shape, pieces, -0.22, 0.18) * drawn
    return jnp.clip(drawn, min=-limit, max=limit).astype(held_as)


def setup_inputs(seed: int = 0) -> dict:
    arg_keys = jax.random.split(jax.random.key(seed), 10)
    return {
        "stash_inputs": draw_stash_inputs(jax.random.fold_in(arg_keys[9], 71), 0),
        "stash_hidden": scatter_about(arg_keys[1], (N_SECTION, STASH, TOK, FF), 1.5, 6.0, ((0, 2), (2, 4), (3, 4))),
        "grad_in": scatter_about(arg_keys[2], (N_SECTION, TOK, D), 1.0, 6.0, ((0, 2), (1, 4), (2, 4))),
        "w_in": scatter_about(arg_keys[3], (N_SECTION, D, FF), D ** -0.5, 0.0546875, ((0, 2), (1, 4), (2, 4))),
        "b_in": scatter_about(arg_keys[4], (N_SECTION, FF), 0.5, 3.0, ((0, 2), (1, 4)), jnp.float32),
        "w_out": scatter_about(arg_keys[5], (N_SECTION, FF, D), FF ** -0.5, 0.0390625, ((0, 2), (1, 4), (2, 4))),
        "b_out": scatter_about(arg_keys[6], (N_SECTION, D), 0.5, 3.0, ((0, 2), (1, 4)), jnp.float32),
        "ln_gain": jnp.clip(1.0 + 0.12 * jax.random.normal(arg_keys[7], (N_SECTION, D), jnp.float32), 0.4, 1.6),
        "plan": draw_plan(jax.random.fold_in(arg_keys[9], 71), 0),
    }


epsilon = 1e-05
root_coef = 0.7978845608028654
cubic_coef = 0.044715

def gelu_value(values):
    inner = root_coef * (values + cubic_coef * values * values * values)
    return 0.5 * values * (1.0 + jnp.tanh(inner))

def gelu_slope(values):
    inner = root_coef * (values + cubic_coef * values * values * values)
    tangent = jnp.tanh(inner)
    return 0.5 * (1.0 + tangent) + 0.5 * values * (1.0 - tangent * tangent) * root_coef * (1.0 + 3.0 * cubic_coef * values * values)

def finish_norm(values, total, squares):
    mean_val = total / D
    sq_mean = squares / D
    inv_std = lax.rsqrt(sq_mean - mean_val * mean_val + epsilon)
    return ((values - mean_val[:, None]) * inv_std[:, None], inv_std)

def transposed(left, right):
    return lax.dot_general(left, right, (((1,), (1,)), ((), ())), preferred_element_type=jnp.float32)

def section_step(fwd_input, bwd_input, bwd_hidden, upstream, w_first, b_first, w_second, b_second, gain_part):
    fwd_hat, fwd_inv = finish_norm(fwd_input, lax.optimization_barrier(jnp.sum(fwd_input, axis=1)), lax.optimization_barrier(jnp.sum(fwd_input * fwd_input, axis=1)))
    bwd_hat, bwd_inv = finish_norm(bwd_input, lax.optimization_barrier(jnp.sum(bwd_input, axis=1)), lax.optimization_barrier(jnp.sum(bwd_input * bwd_input, axis=1)))
    normed = (fwd_hat * gain_part).astype(jnp.bfloat16)
    hidden = jnp.dot(normed, w_first, preferred_element_type=jnp.float32) + b_first
    saved = hidden.astype(jnp.bfloat16)
    activated = gelu_value(hidden).astype(jnp.bfloat16)
    output = (jnp.dot(activated, w_second, preferred_element_type=jnp.float32) + b_second + fwd_input).astype(jnp.bfloat16)
    slopes = transposed(upstream, w_second)
    hid_grad = (slopes * gelu_slope(bwd_hidden)).astype(jnp.bfloat16)
    scaled = transposed(hid_grad, w_first) * gain_part
    first_mean = lax.optimization_barrier(jnp.sum(scaled, axis=1)) / D
    second_mean = lax.optimization_barrier(jnp.sum(scaled * bwd_hat, axis=1)) / D
    in_grad = upstream.astype(jnp.float32) + bwd_inv[:, None] * (scaled - first_mean[:, None] - bwd_hat * second_mean[:, None])
    return (output, in_grad.astype(jnp.bfloat16), saved)

def reference(stash_inputs, stash_hidden, grad_in, w_in, b_in, w_out, b_out, ln_gain, plan):
    outputs = []
    grads = []
    saves = []
    for section_id in range(N_SECTION):
        bwd_slot = plan[section_id, 0]
        fwd_slot = plan[section_id, 1]
        fwd_input = lax.dynamic_index_in_dim(stash_inputs[section_id], fwd_slot, 0, keepdims=False).astype(jnp.float32)
        bwd_input = lax.dynamic_index_in_dim(stash_inputs[section_id], bwd_slot, 0, keepdims=False).astype(jnp.float32)
        bwd_hidden = lax.dynamic_index_in_dim(stash_hidden[section_id], bwd_slot, 0, keepdims=False).astype(jnp.float32)
        output, in_grad, saved = section_step(fwd_input, bwd_input, bwd_hidden, grad_in[section_id], w_in[section_id], b_in[section_id], w_out[section_id], b_out[section_id], ln_gain[section_id])
        outputs.append(output)
        grads.append(in_grad)
        saves.append(saved)
    act_recv = jnp.stack([outputs[(section_id - 1) % N_SECTION] for section_id in range(N_SECTION)])
    grad_recv = jnp.stack([grads[(section_id + 1) % N_SECTION] for section_id in range(N_SECTION)])
    return (act_recv, grad_recv, jnp.stack(saves))
```

```python
import jax
import jax.numpy as jnp
from jax import lax
from jax.sharding import PartitionSpec as P

D = 12288


epsilon = 1e-05
root_coef = 0.7978845608028654
cubic_coef = 0.044715


def shifted(array, axis, by):
    size = lax.axis_size(axis)
    return lax.ppermute(array, axis, [(i, (i + by) % size) for i in range(size)])


def gelu_value(values):
    inner = root_coef * (values + cubic_coef * values * values * values)
    return 0.5 * values * (1.0 + jnp.tanh(inner))


def gelu_slope(values):
    inner = root_coef * (values + cubic_coef * values * values * values)
    tangent = jnp.tanh(inner)
    return 0.5 * (1.0 + tangent) + 0.5 * values * (1.0 - tangent * tangent) * root_coef * (
        1.0 + 3.0 * cubic_coef * values * values
    )


def finish_norm(values, total, squares):
    mean_val = total / D
    sq_mean = squares / D
    inv_std = lax.rsqrt(sq_mean - mean_val * mean_val + epsilon)
    return ((values - mean_val[:, None]) * inv_std[:, None], inv_std)


def transposed(left, right):
    return lax.dot_general(
        left, right, (((1,), (1,)), ((), ())), preferred_element_type=jnp.float32
    )


def gather_direct(block, axis):
    size = lax.axis_size(axis)
    me = lax.axis_index(axis)
    rows = block.shape[0]
    whole = jnp.zeros((size * rows,) + block.shape[1:], block.dtype)
    whole = lax.dynamic_update_slice_in_dim(whole, block, me * rows, 0)
    for by in range(1, size):
        whole = lax.dynamic_update_slice_in_dim(
            whole, shifted(block, axis, by), ((me - by) % size) * rows, 0
        )
    return whole


def scatter_direct(terms, axis):
    size = lax.axis_size(axis)
    me = lax.axis_index(axis)
    rows = terms.shape[0] // size
    total = lax.dynamic_slice_in_dim(terms, me * rows, rows, 0).astype(jnp.float32)
    for by in range(1, size):
        piece = lax.dynamic_slice_in_dim(terms, ((me + by) % size) * rows, rows, 0)
        total = total + shifted(piece, axis, by).astype(jnp.float32)
    return total


def body(stash_inputs, stash_hidden, grad_in, w_in, b_in, w_out, b_out, ln_gain, plan):
    bwd_slot = plan[0, 0]
    fwd_slot = plan[0, 1]
    fwd_input = lax.dynamic_index_in_dim(stash_inputs[0], fwd_slot, 0, keepdims=False).astype(
        jnp.float32
    )
    bwd_input = lax.dynamic_index_in_dim(stash_inputs[0], bwd_slot, 0, keepdims=False).astype(
        jnp.float32
    )
    bwd_hidden = lax.dynamic_index_in_dim(stash_hidden[0], bwd_slot, 0, keepdims=False).astype(
        jnp.float32
    )
    upstream = grad_in[0]
    w_first = w_in[0]
    b_first = b_in[0]
    w_second = w_out[0]
    b_second = b_out[0]
    gain_part = ln_gain[0]
    upstream_all = lax.all_gather(upstream, "row", axis=0, tiled=True)
    sums = lax.psum(
        (
            jnp.sum(fwd_input, axis=1),
            jnp.sum(fwd_input * fwd_input, axis=1),
            jnp.sum(bwd_input, axis=1),
            jnp.sum(bwd_input * bwd_input, axis=1),
        ),
        "col",
    )
    fwd_hat, fwd_inv = finish_norm(fwd_input, sums[0], sums[1])
    bwd_hat, bwd_inv = finish_norm(bwd_input, sums[2], sums[3])
    normed = (fwd_hat * gain_part).astype(jnp.bfloat16)
    normed_all = gather_direct(normed, "row")
    slope_terms = transposed(upstream_all, w_second).astype(jnp.bfloat16)
    slope_terms, normed_all = lax.optimization_barrier((slope_terms, normed_all))
    slopes = lax.psum_scatter(slope_terms, "col", scatter_dimension=0, tiled=True)
    hidden_terms = jnp.dot(normed_all, w_first, preferred_element_type=jnp.float32).astype(
        jnp.bfloat16
    )
    hidden_pre = lax.psum_scatter(hidden_terms, "col", scatter_dimension=0, tiled=True)
    slopes, hidden_terms = lax.optimization_barrier((slopes, hidden_terms))
    hid_grad = (slopes.astype(jnp.float32) * gelu_slope(bwd_hidden)).astype(jnp.bfloat16)
    hidden_pre, hid_grad = lax.optimization_barrier((hidden_pre, hid_grad))
    hidden = hidden_pre.astype(jnp.float32) + b_first
    saved = hidden.astype(jnp.bfloat16)
    activated = gelu_value(hidden).astype(jnp.bfloat16)
    activated, hid_grad = lax.optimization_barrier((activated, hid_grad))
    activated_all = lax.all_gather(activated, "col", axis=0, tiled=True)
    hid_grad_all = lax.all_gather(hid_grad, "col", axis=0, tiled=True)
    out_terms = jnp.dot(activated_all, w_second, preferred_element_type=jnp.float32)
    out_sum = scatter_direct(out_terms.astype(jnp.bfloat16), "row")
    output = (out_sum + b_second + fwd_input).astype(jnp.bfloat16)
    output, hid_grad_all = lax.optimization_barrier((output, hid_grad_all))
    act_recv = shifted(output, "section", 1)
    back_terms = transposed(hid_grad_all, w_first).astype(jnp.bfloat16)
    norm_grad = lax.psum_scatter(back_terms, "row", scatter_dimension=0, tiled=True)
    scaled = norm_grad.astype(jnp.float32) * gain_part
    grad_sums = lax.psum((jnp.sum(scaled, axis=1), jnp.sum(scaled * bwd_hat, axis=1)), "col")
    first_mean = grad_sums[0] / D
    second_mean = grad_sums[1] / D
    in_grad = upstream.astype(jnp.float32) + bwd_inv[:, None] * (
        scaled - first_mean[:, None] - bwd_hat * second_mean[:, None]
    )
    grad_recv = shifted(in_grad.astype(jnp.bfloat16), "section", -1)
    return (act_recv[None], grad_recv[None], saved[None])


def solution(mesh):
    in_specs = (
        P("section", None, "row", "col"),
        P("section", None, "col", "row"),
        P("section", "row", "col"),
        P("section", "col", "row"),
        P("section", "row"),
        P("section", "row", "col"),
        P("section", "col"),
        P("section", "col"),
        P("section", None),
    )
    out_specs = (P("section", "row", "col"), P("section", "row", "col"), P("section", "col", "row"))
    return jax.shard_map(body, mesh=mesh, in_specs=in_specs, out_specs=out_specs, check_vma=False)
```
